32 devices in a mesh: gx: 4 (over y, x), gy: 2 (over core), gz: 4 (over z).
Axes of the slice: x: 2, y: 2, z: 4, core: 2. Of those that a mesh axis runs over, the one named last changes fastest.
Arguments:
- pair_blocks: float32 [529, 1024], P(None, ('gx', 'gy', 'gz')), may hold values from -6 to 6
- basis_map: float32 [529, 64], replicated, may hold values from -0.25 to 0.25
- pair_cells: int32 [3, 1024], P(None, ('gx', 'gy', 'gz')), may hold values from 0 to 511, as said below
- pair_offsets: float32 [3, 1024], P(None, ('gx', 'gy', 'gz')), may hold values from 0 to 1
- exponent_index: int32 [1024], P(('gx', 'gy', 'gz')), may hold values from 0 to 15
- radius_index: int32 [1024], P(('gx', 'gy', 'gz')), may hold values from 0 to 4
- exponents: float32 [16], replicated, may hold values from 7 to 9
Outputs:
- density: float32 [32, 64, 512], P('gx', 'gy', 'gz')
- spectrum: float32 [2, 512, 64, 32], P(None, ('gy', 'gz'), 'gx')
The draws below stay inside these ranges and needn't reach their ends.
Inputs may be any that keep to these rules, and one draw needn't show every extreme that they name: The y of pair_cells column p lies among the 32 cells, and its z among the 128 cells, of the gy and gz index of the device that holds column p. Of the pairs that one device holds at most 16 have x in the same run of 8 cells that one gx index holds, and in every draw some such run gets exactly 16 from every device.
All inputs are finite; a program needn't handle non-finite values.
Results may differ from the reference program's by a relative error of at most 0.0003.
Values sent between devices are 32-bit elements; how exact they have to be, the bound alone decides.
No kernel may reach another device: no remote copies, remote signals or barrier semaphores. Data moves between devices by JAX's collectives and lax.ppermute only.
A program may use at most 64 MiB of HBM per device.

```python
import math
import jax
import jax.numpy as jnp
from jax import lax

BLOCK = 23
DEG = 3
NPOLY = 64
NEXP = 16
HALO = 8
CX = 8
CY = 32
CZ = 128
PAIR_DEV = 32
CAP = 16
PAIRS = 1024
NX = 32
NY = 64
NZ = 512
N_GX = 4
N_GY = 2
N_GZ = 4


def draw_pair_cells(key, part):
    source_count = N_GX * N_GY * N_GZ
    slot_count = N_GX * CAP
    key_level, key_top, key_pick, key_perm, key_x, key_y, key_z = jax.random.split(key, 7)
    levels = jax.random.randint(key_level, (N_GX,), 0, 4)
    favourite = jax.random.randint(key_top, (), 0, N_GX)
    levels = jnp.where(jnp.arange(N_GX) == favourite, 4, levels)
    sources = jnp.arange(source_count, dtype=jnp.int32)
    slot_ids = jnp.arange(slot_count, dtype=jnp.int32)
    slot_target = slot_ids // CAP
    first_slot = slot_ids % CAP == 0
    edge_class = (slot_target[None, :] + sources[:, None]) % 4
    upper_edge = first_slot[None, :] & (edge_class == 0)
    lower_edge = first_slot[None, :] & (edge_class == 2)
    slot_levels = jnp.where(upper_edge | lower_edge, 5, levels[slot_target][None, :])
    noise = jax.random.randint(key_pick, (source_count, slot_count), 0, 65536)
    scores = (slot_levels * 65536 + noise) * slot_count + slot_ids[None, :]
    unused, chosen = lax.top_k(scores, PAIR_DEV)
    orders = jax.vmap(lambda sub_key: jax.random.permutation(sub_key, PAIR_DEV))(jax.random.split(key_perm, source_count))
    chosen = jnp.take_along_axis(chosen, orders, 1)
    targets = chosen // CAP
    chosen_upper = jnp.take_along_axis(upper_edge, chosen, 1)
    chosen_lower = jnp.take_along_axis(lower_edge, chosen, 1)
    source_y = sources // N_GZ % N_GY
    source_z = sources % N_GZ
    inner_x = jax.random.randint(key_x, (source_count, PAIR_DEV), 0, CX)
    inner_x = jnp.where(chosen_upper, CX - 1, jnp.where(chosen_lower, 0, inner_x))
    cells_x = targets * CX + inner_x
    cells_y = source_y[:, None] * CY + jax.random.randint(key_y, (source_count, PAIR_DEV), 0, CY)
    cells_z = source_z[:, None] * CZ + jax.random.randint(key_z, (source_count, PAIR_DEV), 0, CZ)
    return jnp.stack([cells_x, cells_y, cells_z]).reshape(3, source_count * PAIR_DEV).astype(jnp.int32)


def set_ends(entries, own_key, low, high):
    extent = entries.shape
    place = [jax.random.randint(jax.random.fold_in(own_key, axis), (), 0, extent[axis]) for axis in range(len(extent))]
    entries = entries.at[tuple(place)].set(low)
    longest = extent.index(max(extent))
    place[longest] = (place[longest] + 1) % extent[longest]
    return entries.at[tuple(place)].set(high)


def steps_of(stream_key, dims, cuts, low, largest):
    level = 1.0
    for position, blocks in cuts:
        steps = jax.random.uniform(jax.random.fold_in(jax.random.fold_in(stream_key, 6), position), (blocks,), jnp.float32, low / len(cuts), largest / len(cuts))
        level = level * jnp.repeat(jnp.exp(steps), dims[position] // blocks).reshape((-1,) + (1,) * (len(dims) - 1 - position))
    return level


def centred(rng, dims, scale, limit, shards=(), kind=jnp.bfloat16):
    factor_of = steps_of(rng, dims, shards, -0.22, 0.18) if shards else 1.0
    entries = jax.random.normal(rng, dims, jnp.float32) * scale * factor_of
    return jnp.minimum(jnp.maximum(entries, -limit), limit).astype(kind)


def setup_inputs(seed: int = 0) -> dict:
    seeds = jax.random.split(jax.random.key(seed), 8)
    pair_blocks = centred(seeds[0], (BLOCK * BLOCK, PAIRS), 1.0, 6.0, ((1, 32),), jnp.float32)
    basis_map = centred(seeds[1], (BLOCK * BLOCK, NPOLY), (BLOCK * BLOCK) ** -0.5, 0.25, (), jnp.float32)
    pair_cells = draw_pair_cells(jax.random.fold_in(seeds[7], 71), 0)
    pair_offsets = jnp.clip(1.0 * jax.random.uniform(seeds[3], (3, PAIRS), jnp.float32) ** steps_of(seeds[3], (3, PAIRS), ((1, 32),), -0.2, 0.2), 0.0, 1.0)
    exponent_index = set_ends(jax.random.randint(seeds[4], (PAIRS,), 0, NEXP), jax.random.fold_in(seeds[4], 1), 0, NEXP - 1).astype(jnp.int32)
    radius_index = set_ends(jax.random.randint(seeds[5], (PAIRS,), 0, HALO // 2 + 1), jax.random.fold_in(seeds[5], 1), 0, (HALO // 2 + 1) - 1).astype(jnp.int32)
    exponents = jnp.clip(jnp.exp(jax.random.uniform(seeds[6], (NEXP,), jnp.float32, math.log(7.0), math.log(9.0))), 7.0, 9.0)
    return dict(pair_blocks=pair_blocks, basis_map=basis_map, pair_cells=pair_cells, pair_offsets=pair_offsets, exponent_index=exponent_index, radius_index=radius_index, exponents=exponents)


highest = lax.Precision.HIGHEST


def pair_factors(offsets_row, exponent_values, radius_cells):
    span = jnp.arange(2 * HALO + 1, dtype=jnp.int32) - HALO
    distance = span[None, :].astype(jnp.float32) - offsets_row[:, None]
    inside = (jnp.abs(span)[None, :] <= radius_cells[:, None]).astype(jnp.float32)
    envelope = jnp.exp(-exponent_values[:, None] * distance * distance) * inside
    scaled = distance / HALO
    return jnp.stack([scaled ** degree * envelope for degree in range(DEG + 1)], 1)


def reference(pair_blocks, basis_map, pair_cells, pair_offsets, exponent_index, radius_index, exponents):
    side = DEG + 1
    pair_total = pair_blocks.shape[1]
    group_size = 64
    group_count = pair_total // group_size
    coefficients = jnp.dot(basis_map.T, pair_blocks, precision=highest)
    radius_cells = HALO - radius_index
    radius_float = radius_cells.astype(jnp.float32)
    exponent_values = exponents[exponent_index] / (radius_float * radius_float)
    span = jnp.arange(2 * HALO + 1, dtype=jnp.int32) - HALO

    def regroup(values):
        return values.reshape((group_count, group_size) + values.shape[1:])

    pieces_all = (regroup(coefficients.T.reshape(pair_total, side, side, side)),
                  regroup(pair_factors(pair_offsets[0], exponent_values, radius_cells)),
                  regroup(pair_factors(pair_offsets[1], exponent_values, radius_cells)),
                  regroup(pair_factors(pair_offsets[2], exponent_values, radius_cells)),
                  regroup(pair_cells.T))

    def add_group(density_grid, pieces):
        pair_coefs, along_x, along_y, along_z, centre_cells = pieces
        partial_z = jnp.einsum('sijk,skc->sijc', pair_coefs, along_z, precision=highest)
        partial_y = jnp.einsum('sjb,sijc->sibc', along_y, partial_z, precision=highest)
        tile_values = jnp.einsum('sia,sibc->sabc', along_x, partial_y, precision=highest)
        rows_x = (centre_cells[:, 0:1] + span[None, :]) % NX
        rows_y = (centre_cells[:, 1:2] + span[None, :]) % NY
        rows_z = (centre_cells[:, 2:3] + span[None, :]) % NZ
        density_grid = density_grid.at[rows_x[:, :, None, None], rows_y[:, None, :, None], rows_z[:, None, None, :]].add(tile_values)
        return density_grid, None

    density, unused = lax.scan(add_group, jnp.zeros((NX, NY, NZ), jnp.float32), pieces_all)
    transform = jnp.fft.fftn(jnp.transpose(density, (2, 1, 0)), norm="ortho")
    spectrum = jnp.stack([jnp.real(transform), jnp.imag(transform)]).astype(jnp.float32)
    return density, spectrum
```

```python
import functools
import math

import numpy as np
import jax
import jax.numpy as jnp
from jax import lax
from jax.experimental import pallas as pl
from jax.experimental.pallas import tpu as pltpu
from jax.sharding import PartitionSpec as P

DEG = 3
HALO = 8
CX = 8
CY = 32
CZ = 128
SIDE = DEG + 1
EXTRA = 8

highest = lax.Precision.HIGHEST
high = lax.Precision.HIGH


def lanes_dot(a, b):
    return lax.dot_general(
        a, b, (((1,), (1,)), ((), ())), precision=high, preferred_element_type=jnp.float32
    )


def plain_dot(a, b):
    return lax.dot_general(
        a, b, (((1,), (0,)), ((), ())), precision=high, preferred_element_type=jnp.float32
    )


def pack_kernel(table, basis, blocks, cells, offsets, exponent_index, radius_index, out):
    npoly = basis.shape[0]
    out[0:npoly, :] = lanes_dot(basis[...], blocks[...])
    radius = (HALO - radius_index[...]).astype(jnp.float32)
    chosen = exponent_index[...]
    value = jnp.zeros(chosen.shape, jnp.float32)
    for row in range(table.shape[0]):
        value = jnp.where(chosen == row, table[row], value)
    out[npoly : npoly + 3, :] = cells[...].astype(jnp.float32)
    out[npoly + 3 : npoly + 6, :] = offsets[...]
    out[npoly + 6 : npoly + 7, :] = value / (radius * radius)
    out[npoly + 7 : npoly + 8, :] = radius


def factor_rows(coordinate, cell, offset, rate, radius, period):
    steps = coordinate - cell
    if period is not None:
        half = period / 2.0
        steps = jnp.where(steps > half, steps - period, steps)
        steps = jnp.where(steps < -half, steps + period, steps)
    distance = steps - offset
    envelope = jnp.exp(-rate * distance * distance)
    envelope = jnp.where(jnp.abs(steps) <= radius, envelope, 0.0)
    scaled = distance / HALO
    rows = [envelope]
    for degree in range(DEG):
        rows.append(rows[-1] * scaled)
    return rows


def collocate_kernel(anchor, pieces, out, *, period_x, period_y):
    npoly = SIDE**3
    joined = jnp.concatenate([pieces[b] for b in range(pieces.shape[0])], axis=1)
    count = joined.shape[1]

    def row(index):
        return joined[index : index + 1, :]

    rate = row(npoly + 6)
    radius = row(npoly + 7)

    def coordinates(extent, start):
        index = lax.broadcasted_iota(jnp.int32, (extent, count), 0)
        return (index + start).astype(jnp.float32)

    extent_z = CZ + 2 * HALO
    along_x = factor_rows(
        coordinates(CX, anchor[0]), row(npoly), row(npoly + 3), rate, radius, period_x
    )
    along_y = factor_rows(
        coordinates(CY, anchor[1]), row(npoly + 1), row(npoly + 4), rate, radius, period_y
    )
    along_z = factor_rows(
        coordinates(extent_z, anchor[2] - HALO), row(npoly + 2), row(npoly + 5), rate, radius, None
    )
    y_all = jnp.concatenate(along_y, axis=1)
    total = None
    for i in range(SIDE):
        mixed = []
        for j in range(SIDE):
            part = None
            for k in range(SIDE):
                term = along_z[k] * row((i * SIDE + j) * SIDE + k)
                part = term if part is None else part + term
            mixed.append(part)
        x_all = jnp.concatenate([along_x[i]] * SIDE, axis=1)
        outer = (x_all[:, None, :] * y_all[None, :, :]).reshape(CX * CY, SIDE * count)
        product = lanes_dot(outer, jnp.concatenate(mixed, axis=1))
        total = product if total is None else total + product
    total = total.reshape(CX, CY, extent_z)

    @pl.when(pl.program_id(0) == 0)
    def first():
        out[...] = total

    @pl.when(pl.program_id(0) != 0)
    def later():
        out[...] += total


def swap_parts(values, half):
    width = 2 * half
    tiles = []
    for t in range(values.shape[1] // width):
        tiles.append(pltpu.roll(values[:, t * width : (t + 1) * width], half, 1))
    swapped = jnp.concatenate(tiles, axis=1) if len(tiles) > 1 else tiles[0]
    lane = lax.broadcasted_iota(jnp.int32, values.shape, 1) % width
    return jnp.where(lane < half, swapped, -swapped)


def plane_kernel(pieces, table_z, table_y, out, *, groups_y, groups_z, half):
    total = None
    for g in range(groups_z):
        rows = jnp.concatenate([pieces[r * groups_z + g] for r in range(groups_y)], axis=0)
        product = plain_dot(rows, table_z[g])
        total = product if total is None else total + product
    both = jnp.concatenate([total, swap_parts(total, half)], axis=0)
    result = plain_dot(table_y[...], both)
    groups_x, chunks, ky, width = out.shape
    for g in range(groups_x):
        for c in range(chunks):
            out[g, c] = result[g * ky : (g + 1) * ky, c * width : (c + 1) * width]


def lines_kernel(pieces, table_x, out, *, half):
    ky = pieces.shape[1]
    width = 2 * half
    values = jnp.concatenate([pieces[:, q, :] for q in range(ky)], axis=1)
    both = jnp.concatenate([values, swap_parts(values, half)], axis=0)
    result = plain_dot(table_x[...], both)
    for q in range(ky):
        out[0, q] = result[:, q * width : q * width + half]
        out[1, q] = result[:, q * width + half : (q + 1) * width]


def vmem_call(kernel, shape):
    return pl.pallas_call(kernel, out_shape=jax.ShapeDtypeStruct(shape, jnp.float32))


def angle_parts(rows, columns, length):
    product = (rows[:, None].astype(np.int64) * columns[None, :]) % length
    angles = product.astype(np.float64) * (2.0 * math.pi / length)
    factor = 1.0 / math.sqrt(length)
    return np.cos(angles) * factor, np.sin(angles) * factor


def pair_table(length):
    index = np.arange(length)
    cosine, sine = angle_parts(index, index, length)
    return np.concatenate([cosine, sine], axis=1).astype(np.float32)


def depth_table(groups, length, chunk):
    cells = (np.arange(groups)[:, None] * CZ - HALO + np.arange(CZ + 2 * HALO)[None, :]) % length
    cosine, sine = angle_parts(cells.reshape(-1), np.arange(length), length)
    both = np.stack(
        [cosine.reshape(-1, length // chunk, chunk), -sine.reshape(-1, length // chunk, chunk)], 2
    )
    return both.reshape(groups, CZ + 2 * HALO, 2 * length).astype(np.float32)


def dft_parts(length):
    indices = jnp.arange(length, dtype=jnp.int32)
    product = indices[:, None] * indices[None, :] % length
    angles = product.astype(jnp.float32) * (2.0 * math.pi / length)
    factor = 1.0 / math.sqrt(length)
    return (jnp.cos(angles) * factor, jnp.sin(angles) * factor)


def shifts(count):
    forward = [(i, (i + 1) % count) for i in range(count)]
    backward = [(target, source) for source, target in forward]
    return forward, backward


def spectrum_by_axes(density):
    depth_local = lax.all_to_all(density, "gz", split_axis=1, concat_axis=2, tiled=True)
    depth_size = depth_local.shape[2]
    cosine_z, sine_z = dft_parts(depth_size)
    real_z = jnp.einsum("xyz,zk->xyk", depth_local, cosine_z, precision=highest)
    imag_z = -jnp.einsum("xyz,zk->xyk", depth_local, sine_z, precision=highest)
    section_z = jnp.stack([real_z, imag_z])
    rows_devices = lax.axis_size("gy")
    depth_devices = lax.axis_size("gz")
    depth_piece = depth_size // (rows_devices * depth_devices)
    split_view = section_z.reshape(
        2, CX, 1, 1, section_z.shape[2], rows_devices, depth_devices, depth_piece
    )
    moved_rows = lax.all_to_all(
        lax.all_to_all(split_view, "gy", split_axis=5, concat_axis=2, tiled=True),
        "gz",
        split_axis=6,
        concat_axis=3,
        tiled=True,
    )
    rows_local = moved_rows.reshape(2, CX, -1, depth_piece)
    cosine_y, sine_y = dft_parts(rows_local.shape[2])
    real_in = rows_local[0]
    imag_in = rows_local[1]
    real_y = jnp.einsum("xyk,yl->klx", real_in, cosine_y, precision=highest) + jnp.einsum(
        "xyk,yl->klx", imag_in, sine_y, precision=highest
    )
    imag_y = jnp.einsum("xyk,yl->klx", imag_in, cosine_y, precision=highest) - jnp.einsum(
        "xyk,yl->klx", real_in, sine_y, precision=highest
    )
    section_y = jnp.stack([real_y, imag_y])
    width_local = lax.all_to_all(section_y, "gx", split_axis=2, concat_axis=3, tiled=True)
    cosine_x, sine_x = dft_parts(width_local.shape[3])
    real_w = width_local[0]
    imag_w = width_local[1]
    real_x = jnp.einsum("kyx,xm->kym", real_w, cosine_x, precision=highest) + jnp.einsum(
        "kyx,xm->kym", imag_w, sine_x, precision=highest
    )
    imag_x = jnp.einsum("kyx,xm->kym", imag_w, cosine_x, precision=highest) - jnp.einsum(
        "kyx,xm->kym", real_w, sine_x, precision=highest
    )
    return jnp.stack([real_x, imag_x])


def spectrum_by_planes(extended):
    groups_x = lax.axis_size("gx")
    groups_y = lax.axis_size("gy")
    groups_z = lax.axis_size("gz")
    chunks = groups_y * groups_z
    size_x, size_y, size_z = groups_x * CX, groups_y * CY, groups_z * CZ
    half = size_z // chunks
    ky = size_y // groups_x
    planes = lax.all_to_all(extended, ("gy", "gz"), 0, 0, tiled=True)
    sent = vmem_call(
        functools.partial(plane_kernel, groups_y=groups_y, groups_z=groups_z, half=half),
        (groups_x, chunks, ky, 2 * half),
    )(planes, depth_table(groups_z, size_z, half), pair_table(size_y))
    lines = lax.all_to_all(
        sent.reshape(groups_x * chunks, ky, 2 * half), ("gx", "gy", "gz"), 0, 0, tiled=True
    )
    result = vmem_call(functools.partial(lines_kernel, half=half), (2, ky, size_x, half))(
        lines, pair_table(size_x)
    )
    return jnp.transpose(result, (0, 3, 1, 2))


def shards(
    pair_blocks, basis_map, pair_cells, pair_offsets, exponent_index, radius_index, exponents
):
    pair_dev = pair_blocks.shape[1]
    npoly = basis_map.shape[1]
    groups_x = lax.axis_size("gx")
    groups_y = lax.axis_size("gy")
    groups_z = lax.axis_size("gz")
    in_vmem = pl.BlockSpec(memory_space=pltpu.VMEM)
    packed = pl.pallas_call(
        pack_kernel,
        out_shape=jax.ShapeDtypeStruct((npoly + EXTRA, pair_dev), jnp.float32),
        in_specs=[pl.BlockSpec(memory_space=pltpu.SMEM)] + [in_vmem] * 6,
    )(
        exponents,
        basis_map.T,
        pair_blocks.T,
        pair_cells,
        pair_offsets,
        exponent_index[None, :],
        radius_index[None, :],
    )
    if groups_y <= 2:
        gathered = lax.all_gather(packed, ("gx", "gy"))
    else:
        column = lax.all_gather(packed, "gx")
        forward, backward = shifts(groups_y)
        gathered = jnp.concatenate(
            [column, lax.ppermute(column, "gy", forward), lax.ppermute(column, "gy", backward)], 0
        )
    blocks = gathered.shape[0]
    step = 8 if blocks % 8 == 0 else blocks
    anchor = jnp.stack(
        [lax.axis_index("gx") * CX, lax.axis_index("gy") * CY, lax.axis_index("gz") * CZ]
    ).astype(jnp.int32)
    extent_z = CZ + 2 * HALO
    extended = pl.pallas_call(
        functools.partial(
            collocate_kernel, period_x=float(groups_x * CX), period_y=float(groups_y * CY)
        ),
        out_shape=jax.ShapeDtypeStruct((CX, CY, extent_z), jnp.float32),
        grid=(blocks // step,),
        in_specs=[
            pl.BlockSpec(memory_space=pltpu.SMEM),
            pl.BlockSpec((step, npoly + EXTRA, pair_dev), lambda g: (g, 0, 0)),
        ],
        out_specs=pl.BlockSpec((CX, CY, extent_z), lambda g: (0, 0, 0)),
    )(anchor, gathered)
    forward, backward = shifts(groups_z)
    below = lax.ppermute(extended[:, :, CZ + HALO :], "gz", forward)
    above = lax.ppermute(extended[:, :, :HALO], "gz", backward)
    density = (
        extended[:, :, HALO : HALO + CZ]
        + jnp.pad(below, ((0, 0), (0, 0), (0, CZ - HALO)))
        + jnp.pad(above, ((0, 0), (0, 0), (CZ - HALO, 0)))
    )
    chunks = groups_y * groups_z
    aligned = CX == chunks and (2 * groups_z * CZ // chunks) % 128 == 0
    aligned = aligned and (groups_y * CY // groups_x) % 8 == 0
    spectrum = spectrum_by_planes(extended) if aligned else spectrum_by_axes(density)
    return (density, spectrum)


def solution(mesh):
    placed = (
        P(None, ("gx", "gy", "gz")),
        P(),
        P(None, ("gx", "gy", "gz")),
        P(None, ("gx", "gy", "gz")),
        P(("gx", "gy", "gz")),
        P(("gx", "gy", "gz")),
        P(),
    )
    return jax.shard_map(
        shards,
        mesh=mesh,
        in_specs=placed,
        out_specs=(P("gx", "gy", "gz"), P(None, ("gy", "gz"), "gx", None)),
        check_vma=False,
    )
```

```python
import functools
import math

import numpy as np
import jax
import jax.numpy as jnp
from jax import lax
from jax.experimental import pallas as pl
from jax.experimental.pallas import tpu as pltpu
from jax.sharding import PartitionSpec as P

DEG = 3
HALO = 8
CX = 8
CY = 32
CZ = 128
SIDE = DEG + 1
EXTRA = 8

highest = lax.Precision.HIGHEST
high = lax.Precision.HIGH


def lanes_dot(a, b):
    return lax.dot_general(
        a, b, (((1,), (1,)), ((), ())), precision=high, preferred_element_type=jnp.float32
    )


def plain_dot(a, b):
    return lax.dot_general(
        a, b, (((1,), (0,)), ((), ())), precision=high, preferred_element_type=jnp.float32
    )


def pack_kernel(table, basis, blocks, cells, offsets, exponent_index, radius_index, out):
    coefficients = lanes_dot(basis[...], blocks[...])
    radius = (HALO - radius_index[...]).astype(jnp.float32)
    chosen = exponent_index[...]
    value = jnp.zeros(chosen.shape, jnp.float32)
    for row in range(table.shape[0]):
        value = jnp.where(chosen == row, table[row], value)
    values = jnp.concatenate(
        [
            coefficients,
            cells[...].astype(jnp.float32),
            offsets[...],
            value / (radius * radius),
            radius,
        ],
        axis=0,
    )
    if len(out.shape) == 2:
        out[...] = values
    else:
        copies, rows, width = out.shape
        count = values.shape[1]
        groups = values.shape[0] // rows
        spare = [jnp.zeros((rows, width - groups * count), jnp.float32)]
        parts = [values[g * rows : (g + 1) * rows] for g in range(groups)]
        dense = jnp.concatenate(parts + (spare if width > groups * count else []), axis=1)
        for c in range(copies):
            out[c] = dense


def factor_rows(coordinate, cell, offset, rate, radius, period):
    steps = coordinate - cell
    if period is not None:
        half = period / 2.0
        steps = jnp.where(steps > half, steps - period, steps)
        steps = jnp.where(steps < -half, steps + period, steps)
    distance = steps - offset
    envelope = jnp.exp(-rate * distance * distance)
    envelope = jnp.where(jnp.abs(steps) <= radius, envelope, 0.0)
    scaled = distance / HALO
    rows = [envelope]
    for degree in range(DEG):
        rows.append(rows[-1] * scaled)
    return rows


def collocate_kernel(anchor, pieces, out, *, period_x, period_y):
    npoly = SIDE**3
    joined = jnp.concatenate([pieces[b] for b in range(pieces.shape[0])], axis=1)
    count = joined.shape[1]

    def row(index):
        return joined[index : index + 1, :]

    rate = row(npoly + 6)
    radius = row(npoly + 7)

    def coordinates(extent, start):
        index = lax.broadcasted_iota(jnp.int32, (extent, count), 0)
        return (index + start).astype(jnp.float32)

    extent_z = CZ + 2 * HALO
    along_x = factor_rows(
        coordinates(CX, anchor[0]), row(npoly), row(npoly + 3), rate, radius, period_x
    )
    along_y = factor_rows(
        coordinates(CY, anchor[1]), row(npoly + 1), row(npoly + 4), rate, radius, period_y
    )
    along_z = factor_rows(
        coordinates(extent_z, anchor[2] - HALO), row(npoly + 2), row(npoly + 5), rate, radius, None
    )
    y_all = jnp.concatenate(along_y, axis=1)
    total = None
    for i in range(SIDE):
        mixed = []
        for j in range(SIDE):
            part = None
            for k in range(SIDE):
                term = along_z[k] * row((i * SIDE + j) * SIDE + k)
                part = term if part is None else part + term
            mixed.append(part)
        x_all = jnp.concatenate([along_x[i]] * SIDE, axis=1)
        outer = (x_all[:, None, :] * y_all[None, :, :]).reshape(CX * CY, SIDE * count)
        product = lanes_dot(outer, jnp.concatenate(mixed, axis=1))
        total = product if total is None else total + product
    total = total.reshape(CX, CY, extent_z)

    @pl.when(pl.program_id(0) == 0)
    def first():
        out[...] = total

    @pl.when(pl.program_id(0) != 0)
    def later():
        out[...] += total


def joined_pairs(pieces, sources, count):
    rows = pieces.shape[1]
    groups = (SIDE**3 + EXTRA) // rows
    loaded = [pieces[source] for source in sources]
    return jnp.concatenate(
        [
            jnp.concatenate([part[:, g * count : (g + 1) * count] for part in loaded], axis=1)
            for g in range(groups)
        ],
        axis=0,
    )


def cell_range(start, extent, count):
    index = lax.broadcasted_iota(jnp.int32, (extent, count), 0)
    return (index + start).astype(jnp.float32)


def along(joined, axis, coordinate, period):
    base = SIDE**3

    def row(index):
        return joined[base + index : base + index + 1, :]

    return factor_rows(coordinate, row(axis), row(3 + axis), row(6), row(7), period)


def weighted(along_z, joined, first):
    part = None
    for k in range(SIDE):
        term = along_z[k] * joined[first + k : first + k + 1, :]
        part = term if part is None else part + term
    return part


def group_sources(groups_x, groups_y, groups_z, group):
    return [(x * groups_y + y) * groups_z + group for x in range(groups_x) for y in range(groups_y)]


def block_kernel(anchor, pieces, out, *, groups, count):
    groups_x, groups_y, groups_z = groups
    period_x, period_y = float(groups_x * CX), float(groups_y * CY)
    own = anchor[2]

    def load(group):
        joined = joined_pairs(pieces, group_sources(groups_x, groups_y, groups_z, group), count)
        lanes = joined.shape[1]
        along_x = along(joined, 0, cell_range(anchor[0] * CX, CX, lanes), period_x)
        along_y = along(joined, 1, cell_range(anchor[1] * CY, CY, lanes), period_y)
        return joined, lanes, along_x, jnp.concatenate(along_y, axis=1)

    joined, lanes, along_x, y_all = load(own)
    along_z = along(joined, 2, cell_range(own * CZ, CZ, lanes), None)
    total = None
    for i in range(SIDE):
        mixed = [weighted(along_z, joined, (i * SIDE + j) * SIDE) for j in range(SIDE)]
        x_all = jnp.concatenate([along_x[i]] * SIDE, axis=1)
        outer = (x_all[:, None, :] * y_all[None, :, :]).reshape(CX * CY, SIDE * lanes)
        product = lanes_dot(outer, jnp.concatenate(mixed, axis=1))
        total = product if total is None else total + product
    out[...] = total.reshape(CX, CY, CZ)

    def rim(group, first_cell, place):
        joined, lanes, along_x, y_all = load(group)
        along_z = along(joined, 2, cell_range(first_cell, HALO, lanes), None)
        columns = []
        for j in range(SIDE):
            column = None
            for i in range(SIDE):
                mixed = weighted(along_z, joined, (i * SIDE + j) * SIDE)
                term = along_x[i][:, None, :] * mixed[None, :, :]
                column = term if column is None else column + term
            columns.append(column.reshape(CX * HALO, lanes))
        product = lanes_dot(y_all, jnp.concatenate(columns, axis=1))
        for x in range(CX):
            out[x, :, place : place + HALO] += product[:, x * HALO : (x + 1) * HALO]

    before = (own + groups_z - 1) % groups_z
    after = (own + 1) % groups_z
    rim(before, (before + 1) * CZ, 0)
    rim(after, after * CZ - HALO, CZ - HALO)


def swap_parts(values, half):
    width = 2 * half
    tiles = []
    for t in range(values.shape[1] // width):
        tiles.append(pltpu.roll(values[:, t * width : (t + 1) * width], half, 1))
    swapped = jnp.concatenate(tiles, axis=1) if len(tiles) > 1 else tiles[0]
    lane = lax.broadcasted_iota(jnp.int32, values.shape, 1) % width
    return jnp.where(lane < half, swapped, -swapped)


def plane_kernel(anchor, pieces, table_z, table_y, out, *, groups, count, half):
    groups_x, groups_y, groups_z = groups
    period_x, period_y = float(groups_x * CX), float(groups_y * CY)
    plane = anchor[0] * CX + anchor[1] * groups_z + anchor[2]
    total = None
    for g in range(groups_z):
        joined = joined_pairs(pieces, group_sources(groups_x, groups_y, groups_z, g), count)
        lanes = joined.shape[1]
        along_x = along(joined, 0, cell_range(plane, 1, lanes), period_x)
        along_y = along(joined, 1, cell_range(0, groups_y * CY, lanes), period_y)
        along_z = along(joined, 2, cell_range(g * CZ - HALO, CZ + 2 * HALO, lanes), None)
        square = SIDE * SIDE
        crossed = None
        for i in range(SIDE):
            term = along_x[i] * joined[i * square : (i + 1) * square, :]
            crossed = term if crossed is None else crossed + term
        mixed = [weighted(along_z, crossed, j * SIDE) for j in range(SIDE)]
        rows = lanes_dot(jnp.concatenate(along_y, axis=1), jnp.concatenate(mixed, axis=1))
        product = plain_dot(rows, table_z[g])
        total = product if total is None else total + product
    both = jnp.concatenate([total, swap_parts(total, half)], axis=0)
    result = plain_dot(table_y[...], both)
    ky, width = out.shape[1:]
    chunks = groups_y * groups_z
    for g in range(groups_x):
        for c in range(chunks):
            out[g * chunks + c] = result[g * ky : (g + 1) * ky, c * width : (c + 1) * width]


def lines_kernel(pieces, table_x, out, *, half):
    ky = pieces.shape[1]
    width = 2 * half
    values = jnp.concatenate([pieces[:, q, :] for q in range(ky)], axis=1)
    both = jnp.concatenate([values, swap_parts(values, half)], axis=0)
    result = plain_dot(table_x[...], both)
    for q in range(ky):
        out[0, q] = result[:, q * width : q * width + half]
        out[1, q] = result[:, q * width + half : (q + 1) * width]


def vmem_call(kernel, shape, spaces):
    return pl.pallas_call(
        kernel,
        out_shape=jax.ShapeDtypeStruct(shape, jnp.float32),
        in_specs=[pl.BlockSpec(memory_space=space) for space in spaces],
        out_specs=pl.BlockSpec(memory_space=pltpu.VMEM),
    )


def angle_parts(rows, columns, length):
    product = (rows[:, None].astype(np.int64) * columns[None, :]) % length
    angles = product.astype(np.float64) * (2.0 * math.pi / length)
    factor = 1.0 / math.sqrt(length)
    return np.cos(angles) * factor, np.sin(angles) * factor


def pair_table(length):
    index = np.arange(length)
    cosine, sine = angle_parts(index, index, length)
    return np.concatenate([cosine, sine], axis=1).astype(np.float32)


def depth_table(groups, length, chunk):
    cells = (np.arange(groups)[:, None] * CZ - HALO + np.arange(CZ + 2 * HALO)[None, :]) % length
    cosine, sine = angle_parts(cells.reshape(-1), np.arange(length), length)
    both = np.stack(
        [cosine.reshape(-1, length // chunk, chunk), -sine.reshape(-1, length // chunk, chunk)], 2
    )
    return both.reshape(groups, CZ + 2 * HALO, 2 * length).astype(np.float32)


def dft_parts(length):
    indices = jnp.arange(length, dtype=jnp.int32)
    product = indices[:, None] * indices[None, :] % length
    angles = product.astype(jnp.float32) * (2.0 * math.pi / length)
    factor = 1.0 / math.sqrt(length)
    return (jnp.cos(angles) * factor, jnp.sin(angles) * factor)


def shifts(count):
    forward = [(i, (i + 1) % count) for i in range(count)]
    backward = [(target, source) for source, target in forward]
    return forward, backward


def spectrum_by_axes(density):
    depth_local = lax.all_to_all(density, "gz", split_axis=1, concat_axis=2, tiled=True)
    depth_size = depth_local.shape[2]
    cosine_z, sine_z = dft_parts(depth_size)
    real_z = jnp.einsum("xyz,zk->xyk", depth_local, cosine_z, precision=highest)
    imag_z = -jnp.einsum("xyz,zk->xyk", depth_local, sine_z, precision=highest)
    section_z = jnp.stack([real_z, imag_z])
    rows_devices = lax.axis_size("gy")
    depth_devices = lax.axis_size("gz")
    depth_piece = depth_size // (rows_devices * depth_devices)
    split_view = section_z.reshape(
        2, CX, 1, 1, section_z.shape[2], rows_devices, depth_devices, depth_piece
    )
    moved_rows = lax.all_to_all(
        lax.all_to_all(split_view, "gy", split_axis=5, concat_axis=2, tiled=True),
        "gz",
        split_axis=6,
        concat_axis=3,
        tiled=True,
    )
    rows_local = moved_rows.reshape(2, CX, -1, depth_piece)
    cosine_y, sine_y = dft_parts(rows_local.shape[2])
    real_in = rows_local[0]
    imag_in = rows_local[1]
    real_y = jnp.einsum("xyk,yl->klx", real_in, cosine_y, precision=highest) + jnp.einsum(
        "xyk,yl->klx", imag_in, sine_y, precision=highest
    )
    imag_y = jnp.einsum("xyk,yl->klx", imag_in, cosine_y, precision=highest) - jnp.einsum(
        "xyk,yl->klx", real_in, sine_y, precision=highest
    )
    section_y = jnp.stack([real_y, imag_y])
    width_local = lax.all_to_all(section_y, "gx", split_axis=2, concat_axis=3, tiled=True)
    cosine_x, sine_x = dft_parts(width_local.shape[3])
    real_w = width_local[0]
    imag_w = width_local[1]
    real_x = jnp.einsum("kyx,xm->kym", real_w, cosine_x, precision=highest) + jnp.einsum(
        "kyx,xm->kym", imag_w, sine_x, precision=highest
    )
    imag_x = jnp.einsum("kyx,xm->kym", imag_w, cosine_x, precision=highest) - jnp.einsum(
        "kyx,xm->kym", real_w, sine_x, precision=highest
    )
    return jnp.stack([real_x, imag_x])


def by_planes(pack, groups, pair_dev, anchor):
    groups_x, groups_y, groups_z = groups
    chunks = groups_y * groups_z
    size_x, size_y, size_z = groups_x * CX, groups_y * CY, groups_z * CZ
    half = size_z // chunks
    ky = size_y // groups_x
    everyone = ("gx", "gy", "gz")
    dense = pack((groups_x * chunks, (SIDE**3 + EXTRA) // 3, 128))
    gathered = lax.all_to_all(dense, everyone, 0, 0, tiled=True)
    smem, vmem = pltpu.SMEM, pltpu.VMEM
    sent = vmem_call(
        functools.partial(plane_kernel, groups=groups, count=pair_dev, half=half),
        (groups_x * chunks, ky, 2 * half),
        [smem] + [vmem] * 3,
    )(anchor, gathered, depth_table(groups_z, size_z, half), pair_table(size_y))
    lines = lax.all_to_all(sent, everyone, 0, 0, tiled=True)
    density = vmem_call(
        functools.partial(block_kernel, groups=groups, count=pair_dev),
        (CX, CY, CZ),
        [smem, vmem],
    )(anchor, gathered)
    result = vmem_call(
        functools.partial(lines_kernel, half=half), (2, ky, size_x, half), [vmem] * 2
    )(lines, pair_table(size_x))
    return density, jnp.transpose(result, (0, 3, 1, 2))


def shards(
    pair_blocks, basis_map, pair_cells, pair_offsets, exponent_index, radius_index, exponents
):
    pair_dev = pair_blocks.shape[1]
    npoly = basis_map.shape[1]
    groups_x = lax.axis_size("gx")
    groups_y = lax.axis_size("gy")
    groups_z = lax.axis_size("gz")
    def pack(shape):
        return vmem_call(pack_kernel, shape, [pltpu.SMEM] + [pltpu.VMEM] * 6)(
            exponents,
            basis_map.T,
            pair_blocks.T,
            pair_cells,
            pair_offsets,
            exponent_index[None, :],
            radius_index[None, :],
        )

    chunks = groups_y * groups_z
    aligned = CX == chunks and 2 * groups_z * CZ == 128 * chunks and 3 * pair_dev <= 128
    if aligned and (groups_y * CY // groups_x) % 8 == 0:
        place = jnp.stack([lax.axis_index(name) for name in ("gx", "gy", "gz")])
        sizes = (groups_x, groups_y, groups_z)
        return by_planes(pack, sizes, pair_dev, place.astype(jnp.int32))
    packed = pack((npoly + EXTRA, pair_dev))
    if groups_y <= 2:
        gathered = lax.all_gather(packed, ("gx", "gy"))
    else:
        column = lax.all_gather(packed, "gx")
        forward, backward = shifts(groups_y)
        gathered = jnp.concatenate(
            [column, lax.ppermute(column, "gy", forward), lax.ppermute(column, "gy", backward)], 0
        )
    blocks = gathered.shape[0]
    step = 8 if blocks % 8 == 0 else blocks
    anchor = jnp.stack(
        [lax.axis_index("gx") * CX, lax.axis_index("gy") * CY, lax.axis_index("gz") * CZ]
    ).astype(jnp.int32)
    extent_z = CZ + 2 * HALO
    extended = pl.pallas_call(
        functools.partial(
            collocate_kernel, period_x=float(groups_x * CX), period_y=float(groups_y * CY)
        ),
        out_shape=jax.ShapeDtypeStruct((CX, CY, extent_z), jnp.float32),
        grid=(blocks // step,),
        in_specs=[
            pl.BlockSpec(memory_space=pltpu.SMEM),
            pl.BlockSpec((step, npoly + EXTRA, pair_dev), lambda g: (g, 0, 0)),
        ],
        out_specs=pl.BlockSpec((CX, CY, extent_z), lambda g: (0, 0, 0)),
    )(anchor, gathered)
    forward, backward = shifts(groups_z)
    below = lax.ppermute(extended[:, :, CZ + HALO :], "gz", forward)
    above = lax.ppermute(extended[:, :, :HALO], "gz", backward)
    density = (
        extended[:, :, HALO : HALO + CZ]
        + jnp.pad(below, ((0, 0), (0, 0), (0, CZ - HALO)))
        + jnp.pad(above, ((0, 0), (0, 0), (CZ - HALO, 0)))
    )
    spectrum = spectrum_by_axes(density)
    return (density, spectrum)


def solution(mesh):
    placed = (
        P(None, ("gx", "gy", "gz")),
        P(),
        P(None, ("gx", "gy", "gz")),
        P(None, ("gx", "gy", "gz")),
        P(("gx", "gy", "gz")),
        P(("gx", "gy", "gz")),
        P(),
    )
    return jax.shard_map(
        shards,
        mesh=mesh,
        in_specs=placed,
        out_specs=(P("gx", "gy", "gz"), P(None, ("gy", "gz"), "gx", None)),
        check_vma=False,
    )
```

```python
import functools
import math

import numpy as np
import jax
import jax.numpy as jnp
from jax import lax
from jax.experimental import pallas as pl
from jax.experimental.pallas import tpu as pltpu
from jax.sharding import PartitionSpec as P

DEG = 3
HALO = 8
CX = 8
CY = 32
CZ = 128
SIDE = DEG + 1
EXTRA = 8

highest = lax.Precision.HIGHEST
high = lax.Precision.HIGH


def lanes_dot(a, b):
    return lax.dot_general(
        a, b, (((1,), (1,)), ((), ())), precision=high, preferred_element_type=jnp.float32
    )


def plain_dot(a, b):
    return lax.dot_general(
        a, b, (((1,), (0,)), ((), ())), precision=high, preferred_element_type=jnp.float32
    )


def pack_kernel(table, basis, blocks, cells, offsets, exponent_index, radius_index, out):
    coefficients = lanes_dot(basis[...], blocks[...])
    radius = (HALO - radius_index[...]).astype(jnp.float32)
    chosen = exponent_index[...]
    value = jnp.zeros(chosen.shape, jnp.float32)
    for row in range(table.shape[0]):
        value = jnp.where(chosen == row, table[row], value)
    values = jnp.concatenate(
        [
            coefficients,
            cells[...].astype(jnp.float32),
            offsets[...],
            value / (radius * radius),
            radius,
        ],
        axis=0,
    )
    if len(out.shape) == 2:
        out[...] = values
    else:
        copies, rows, width = out.shape
        count = values.shape[1]
        groups = values.shape[0] // rows
        spare = [jnp.zeros((rows, width - groups * count), jnp.float32)]
        parts = [values[g * rows : (g + 1) * rows] for g in range(groups)]
        dense = jnp.concatenate(parts + (spare if width > groups * count else []), axis=1)
        for c in range(copies):
            out[c] = dense


def factor_rows(coordinate, cell, offset, rate, radius, period):
    steps = coordinate - cell
    if period is not None:
        half = period / 2.0
        steps = jnp.where(steps > half, steps - period, steps)
        steps = jnp.where(steps < -half, steps + period, steps)
    distance = steps - offset
    envelope = jnp.exp(-rate * distance * distance)
    envelope = jnp.where(jnp.abs(steps) <= radius, envelope, 0.0)
    scaled = distance / HALO
    rows = [envelope]
    for degree in range(DEG):
        rows.append(rows[-1] * scaled)
    return rows


def collocate_kernel(anchor, pieces, out, *, period_x, period_y):
    npoly = SIDE**3
    joined = jnp.concatenate([pieces[b] for b in range(pieces.shape[0])], axis=1)
    count = joined.shape[1]

    def row(index):
        return joined[index : index + 1, :]

    rate = row(npoly + 6)
    radius = row(npoly + 7)

    def coordinates(extent, start):
        index = lax.broadcasted_iota(jnp.int32, (extent, count), 0)
        return (index + start).astype(jnp.float32)

    extent_z = CZ + 2 * HALO
    along_x = factor_rows(
        coordinates(CX, anchor[0]), row(npoly), row(npoly + 3), rate, radius, period_x
    )
    along_y = factor_rows(
        coordinates(CY, anchor[1]), row(npoly + 1), row(npoly + 4), rate, radius, period_y
    )
    along_z = factor_rows(
        coordinates(extent_z, anchor[2] - HALO), row(npoly + 2), row(npoly + 5), rate, radius, None
    )
    y_all = jnp.concatenate(along_y, axis=1)
    total = None
    for i in range(SIDE):
        mixed = []
        for j in range(SIDE):
            part = None
            for k in range(SIDE):
                term = along_z[k] * row((i * SIDE + j) * SIDE + k)
                part = term if part is None else part + term
            mixed.append(part)
        x_all = jnp.concatenate([along_x[i]] * SIDE, axis=1)
        outer = (x_all[:, None, :] * y_all[None, :, :]).reshape(CX * CY, SIDE * count)
        product = lanes_dot(outer, jnp.concatenate(mixed, axis=1))
        total = product if total is None else total + product
    total = total.reshape(CX, CY, extent_z)

    @pl.when(pl.program_id(0) == 0)
    def first():
        out[...] = total

    @pl.when(pl.program_id(0) != 0)
    def later():
        out[...] += total


def joined_pairs(pieces, sources, count):
    rows = pieces.shape[1]
    groups = (SIDE**3 + EXTRA) // rows
    loaded = [pieces[source] for source in sources]
    return jnp.concatenate(
        [
            jnp.concatenate([part[:, g * count : (g + 1) * count] for part in loaded], axis=1)
            for g in range(groups)
        ],
        axis=0,
    )


def cell_range(start, extent, count):
    index = lax.broadcasted_iota(jnp.int32, (extent, count), 0)
    return (index + start).astype(jnp.float32)


def along(joined, axis, coordinate, period):
    base = SIDE**3

    def row(index):
        return joined[base + index : base + index + 1, :]

    return factor_rows(coordinate, row(axis), row(3 + axis), row(6), row(7), period)


def weighted(along_z, joined, first):
    part = None
    for k in range(SIDE):
        term = along_z[k] * joined[first + k : first + k + 1, :]
        part = term if part is None else part + term
    return part


def group_sources(groups_x, groups_y, groups_z, group):
    return [(x * groups_y + y) * groups_z + group for x in range(groups_x) for y in range(groups_y)]


def block_kernel(anchor, pieces, out, *, groups, count):
    groups_x, groups_y, groups_z = groups
    period_x, period_y = float(groups_x * CX), float(groups_y * CY)
    own = anchor[2]

    def load(group):
        joined = joined_pairs(pieces, group_sources(groups_x, groups_y, groups_z, group), count)
        lanes = joined.shape[1]
        along_x = along(joined, 0, cell_range(anchor[0] * CX, CX, lanes), period_x)
        along_y = along(joined, 1, cell_range(anchor[1] * CY, CY, lanes), period_y)
        return joined, lanes, along_x, jnp.concatenate(along_y, axis=1)

    joined, lanes, along_x, y_all = load(own)
    along_z = along(joined, 2, cell_range(own * CZ, CZ, lanes), None)
    total = None
    for i in range(SIDE):
        mixed = [weighted(along_z, joined, (i * SIDE + j) * SIDE) for j in range(SIDE)]
        x_all = jnp.concatenate([along_x[i]] * SIDE, axis=1)
        outer = (x_all[:, None, :] * y_all[None, :, :]).reshape(CX * CY, SIDE * lanes)
        product = lanes_dot(outer, jnp.concatenate(mixed, axis=1))
        total = product if total is None else total + product
    out[...] = total.reshape(CX, CY, CZ)

    def rim(group, first_cell, place):
        joined, lanes, along_x, y_all = load(group)
        along_z = along(joined, 2, cell_range(first_cell, HALO, lanes), None)
        columns = []
        for j in range(SIDE):
            column = None
            for i in range(SIDE):
                mixed = weighted(along_z, joined, (i * SIDE + j) * SIDE)
                term = along_x[i][:, None, :] * mixed[None, :, :]
                column = term if column is None else column + term
            columns.append(column.reshape(CX * HALO, lanes))
        product = lanes_dot(y_all, jnp.concatenate(columns, axis=1))
        for x in range(CX):
            out[x, :, place : place + HALO] += product[:, x * HALO : (x + 1) * HALO]

    before = (own + groups_z - 1) % groups_z
    after = (own + 1) % groups_z
    rim(before, (before + 1) * CZ, 0)
    rim(after, after * CZ - HALO, CZ - HALO)


def swap_parts(values, half):
    width = 2 * half
    tiles = []
    for t in range(values.shape[1] // width):
        tiles.append(pltpu.roll(values[:, t * width : (t + 1) * width], half, 1))
    swapped = jnp.concatenate(tiles, axis=1) if len(tiles) > 1 else tiles[0]
    lane = lax.broadcasted_iota(jnp.int32, values.shape, 1) % width
    return jnp.where(lane < half, swapped, -swapped)


def plane_kernel(
    anchor, far_pieces, far_upper, far_lower, table_y, out,
    pieces, upper, lower, sem_pieces, sem_upper, sem_lower, *, groups, count, half
):
    fetch = pltpu.make_async_copy(far_pieces, pieces, sem_pieces)
    fetch.start()
    fetch_upper = pltpu.make_async_copy(far_upper, upper, sem_upper)
    fetch_upper.start()
    fetch_lower = pltpu.make_async_copy(far_lower, lower, sem_lower)
    fetch_lower.start()
    fetch.wait()
    groups_x, groups_y, groups_z = groups
    period_x, period_y = float(groups_x * CX), float(groups_y * CY)
    plane = anchor[0] * CX + anchor[1] * groups_z + anchor[2]
    total = None
    parts = []
    for g in range(groups_z):
        joined = joined_pairs(pieces, group_sources(groups_x, groups_y, groups_z, g), count)
        lanes = joined.shape[1]
        along_x = along(joined, 0, cell_range(plane, 1, lanes), period_x)
        along_y = along(joined, 1, cell_range(0, groups_y * CY, lanes), period_y)
        along_z = along(joined, 2, cell_range(g * CZ - HALO, CZ + 2 * HALO, lanes), None)
        square = SIDE * SIDE
        crossed = None
        for i in range(SIDE):
            term = along_x[i] * joined[i * square : (i + 1) * square, :]
            crossed = term if crossed is None else crossed + term
        mixed = [weighted(along_z, crossed, j * SIDE) for j in range(SIDE)]
        rows = lanes_dot(jnp.concatenate(along_y, axis=1), jnp.concatenate(mixed, axis=1))
        parts.append(split_bf16(rows))
    fetch_upper.wait()
    fetch_lower.wait()
    for g in range(groups_z):
        rows_upper, rows_lower = parts[g]
        product = bf16_dot(rows_upper, upper[g]) + (
            bf16_dot(rows_upper, lower[g]) + bf16_dot(rows_lower, upper[g])
        )
        total = product if total is None else total + product
    both = jnp.concatenate([total, swap_parts(total, half)], axis=0)
    result = plain_dot(table_y[...], both)
    ky, width = out.shape[1:]
    chunks = groups_y * groups_z
    for g in range(groups_x):
        for c in range(chunks):
            out[g * chunks + c] = result[g * ky : (g + 1) * ky, c * width : (c + 1) * width]


def lines_kernel(pieces, table_x, out, *, half):
    ky = pieces.shape[1]
    width = 2 * half
    values = jnp.concatenate([pieces[:, q, :] for q in range(ky)], axis=1)
    both = jnp.concatenate([values, swap_parts(values, half)], axis=0)
    result = plain_dot(table_x[...], both)
    for q in range(ky):
        out[0, q] = result[:, q * width : q * width + half]
        out[1, q] = result[:, q * width + half : (q + 1) * width]


def split_bf16(values):
    upper = values.astype(jnp.bfloat16)
    lower = (values - upper.astype(jnp.float32)).astype(jnp.bfloat16)
    return upper, lower


def bf16_dot(a, b):
    return lax.dot_general(a, b, (((1,), (0,)), ((), ())), preferred_element_type=jnp.float32)


def staged_call(kernel, shape, spaces, scratch):
    copies = [pltpu.SemaphoreType.DMA(()) for _ in scratch]
    return pl.pallas_call(
        kernel,
        out_shape=jax.ShapeDtypeStruct(shape, jnp.float32),
        in_specs=[pl.BlockSpec(memory_space=space) for space in spaces],
        out_specs=pl.BlockSpec(memory_space=pltpu.VMEM),
        scratch_shapes=[pltpu.VMEM(array.shape, array.dtype) for array in scratch] + copies,
    )


def vmem_call(kernel, shape, spaces):
    return pl.pallas_call(
        kernel,
        out_shape=jax.ShapeDtypeStruct(shape, jnp.float32),
        in_specs=[pl.BlockSpec(memory_space=space) for space in spaces],
        out_specs=pl.BlockSpec(memory_space=pltpu.VMEM),
    )


def angle_parts(rows, columns, length):
    product = (rows[:, None].astype(np.int64) * columns[None, :]) % length
    angles = product.astype(np.float64) * (2.0 * math.pi / length)
    factor = 1.0 / math.sqrt(length)
    return np.cos(angles) * factor, np.sin(angles) * factor


def pair_table(length):
    index = np.arange(length)
    cosine, sine = angle_parts(index, index, length)
    return np.concatenate([cosine, sine], axis=1).astype(np.float32)


def depth_table(groups, length, chunk):
    cells = (np.arange(groups)[:, None] * CZ - HALO + np.arange(CZ + 2 * HALO)[None, :]) % length
    cosine, sine = angle_parts(cells.reshape(-1), np.arange(length), length)
    both = np.stack(
        [cosine.reshape(-1, length // chunk, chunk), -sine.reshape(-1, length // chunk, chunk)], 2
    )
    return both.reshape(groups, CZ + 2 * HALO, 2 * length).astype(np.float32)


def dft_parts(length):
    indices = jnp.arange(length, dtype=jnp.int32)
    product = indices[:, None] * indices[None, :] % length
    angles = product.astype(jnp.float32) * (2.0 * math.pi / length)
    factor = 1.0 / math.sqrt(length)
    return (jnp.cos(angles) * factor, jnp.sin(angles) * factor)


def shifts(count):
    forward = [(i, (i + 1) % count) for i in range(count)]
    backward = [(target, source) for source, target in forward]
    return forward, backward


def spectrum_by_axes(density):
    depth_local = lax.all_to_all(density, "gz", split_axis=1, concat_axis=2, tiled=True)
    depth_size = depth_local.shape[2]
    cosine_z, sine_z = dft_parts(depth_size)
    real_z = jnp.einsum("xyz,zk->xyk", depth_local, cosine_z, precision=highest)
    imag_z = -jnp.einsum("xyz,zk->xyk", depth_local, sine_z, precision=highest)
    section_z = jnp.stack([real_z, imag_z])
    rows_devices = lax.axis_size("gy")
    depth_devices = lax.axis_size("gz")
    depth_piece = depth_size // (rows_devices * depth_devices)
    split_view = section_z.reshape(
        2, CX, 1, 1, section_z.shape[2], rows_devices, depth_devices, depth_piece
    )
    moved_rows = lax.all_to_all(
        lax.all_to_all(split_view, "gy", split_axis=5, concat_axis=2, tiled=True),
        "gz",
        split_axis=6,
        concat_axis=3,
        tiled=True,
    )
    rows_local = moved_rows.reshape(2, CX, -1, depth_piece)
    cosine_y, sine_y = dft_parts(rows_local.shape[2])
    real_in = rows_local[0]
    imag_in = rows_local[1]
    real_y = jnp.einsum("xyk,yl->klx", real_in, cosine_y, precision=highest) + jnp.einsum(
        "xyk,yl->klx", imag_in, sine_y, precision=highest
    )
    imag_y = jnp.einsum("xyk,yl->klx", imag_in, cosine_y, precision=highest) - jnp.einsum(
        "xyk,yl->klx", real_in, sine_y, precision=highest
    )
    section_y = jnp.stack([real_y, imag_y])
    width_local = lax.all_to_all(section_y, "gx", split_axis=2, concat_axis=3, tiled=True)
    cosine_x, sine_x = dft_parts(width_local.shape[3])
    real_w = width_local[0]
    imag_w = width_local[1]
    real_x = jnp.einsum("kyx,xm->kym", real_w, cosine_x, precision=highest) + jnp.einsum(
        "kyx,xm->kym", imag_w, sine_x, precision=highest
    )
    imag_x = jnp.einsum("kyx,xm->kym", imag_w, cosine_x, precision=highest) - jnp.einsum(
        "kyx,xm->kym", real_w, sine_x, precision=highest
    )
    return jnp.stack([real_x, imag_x])


def by_planes(pack, groups, pair_dev, anchor):
    groups_x, groups_y, groups_z = groups
    chunks = groups_y * groups_z
    size_x, size_y, size_z = groups_x * CX, groups_y * CY, groups_z * CZ
    half = size_z // chunks
    ky = size_y // groups_x
    everyone = ("gx", "gy", "gz")
    dense = pack((groups_x * chunks, (SIDE**3 + EXTRA) // 3, 128))
    gathered = lax.all_to_all(dense, everyone, 0, 0, tiled=True)
    smem, vmem, free = pltpu.SMEM, pltpu.VMEM, pl.ANY
    table = depth_table(groups_z, size_z, half)
    upper = table.astype(jnp.bfloat16)
    lower = (table - upper.astype(np.float32)).astype(jnp.bfloat16)
    sent = staged_call(
        functools.partial(plane_kernel, groups=groups, count=pair_dev, half=half),
        (groups_x * chunks, ky, 2 * half),
        [smem, free, free, free, vmem],
        [gathered, upper, lower],
    )(anchor, gathered, upper, lower, pair_table(size_y))
    lines = lax.all_to_all(sent, everyone, 0, 0, tiled=True)
    density = vmem_call(
        functools.partial(block_kernel, groups=groups, count=pair_dev),
        (CX, CY, CZ),
        [smem, vmem],
    )(anchor, gathered)
    result = vmem_call(
        functools.partial(lines_kernel, half=half), (2, ky, size_x, half), [vmem] * 2
    )(lines, pair_table(size_x))
    return density, jnp.transpose(result, (0, 3, 1, 2))


def shards(
    pair_blocks, basis_map, pair_cells, pair_offsets, exponent_index, radius_index, exponents
):
    pair_dev = pair_blocks.shape[1]
    npoly = basis_map.shape[1]
    groups_x = lax.axis_size("gx")
    groups_y = lax.axis_size("gy")
    groups_z = lax.axis_size("gz")
    def pack(shape):
        return vmem_call(pack_kernel, shape, [pltpu.SMEM] + [pltpu.VMEM] * 6)(
            exponents,
            basis_map.T,
            pair_blocks.T,
            pair_cells,
            pair_offsets,
            exponent_index[None, :],
            radius_index[None, :],
        )

    chunks = groups_y * groups_z
    aligned = CX == chunks and 2 * groups_z * CZ == 128 * chunks and 3 * pair_dev <= 128
    if aligned and (groups_y * CY // groups_x) % 8 == 0:
        place = jnp.stack([lax.axis_index(name) for name in ("gx", "gy", "gz")])
        sizes = (groups_x, groups_y, groups_z)
        return by_planes(pack, sizes, pair_dev, place.astype(jnp.int32))
    packed = pack((npoly + EXTRA, pair_dev))
    if groups_y <= 2:
        gathered = lax.all_gather(packed, ("gx", "gy"))
    else:
        column = lax.all_gather(packed, "gx")
        forward, backward = shifts(groups_y)
        gathered = jnp.concatenate(
            [column, lax.ppermute(column, "gy", forward), lax.ppermute(column, "gy", backward)], 0
        )
    blocks = gathered.shape[0]
    step = 8 if blocks % 8 == 0 else blocks
    anchor = jnp.stack(
        [lax.axis_index("gx") * CX, lax.axis_index("gy") * CY, lax.axis_index("gz") * CZ]
    ).astype(jnp.int32)
    extent_z = CZ + 2 * HALO
    extended = pl.pallas_call(
        functools.partial(
            collocate_kernel, period_x=float(groups_x * CX), period_y=float(groups_y * CY)
        ),
        out_shape=jax.ShapeDtypeStruct((CX, CY, extent_z), jnp.float32),
        grid=(blocks // step,),
        in_specs=[
            pl.BlockSpec(memory_space=pltpu.SMEM),
            pl.BlockSpec((step, npoly + EXTRA, pair_dev), lambda g: (g, 0, 0)),
        ],
        out_specs=pl.BlockSpec((CX, CY, extent_z), lambda g: (0, 0, 0)),
    )(anchor, gathered)
    forward, backward = shifts(groups_z)
    below = lax.ppermute(extended[:, :, CZ + HALO :], "gz", forward)
    above = lax.ppermute(extended[:, :, :HALO], "gz", backward)
    density = (
        extended[:, :, HALO : HALO + CZ]
        + jnp.pad(below, ((0, 0), (0, 0), (0, CZ - HALO)))
        + jnp.pad(above, ((0, 0), (0, 0), (CZ - HALO, 0)))
    )
    spectrum = spectrum_by_axes(density)
    return (density, spectrum)


def solution(mesh):
    placed = (
        P(None, ("gx", "gy", "gz")),
        P(),
        P(None, ("gx", "gy", "gz")),
        P(None, ("gx", "gy", "gz")),
        P(("gx", "gy", "gz")),
        P(("gx", "gy", "gz")),
        P(),
    )
    return jax.shard_map(
        shards,
        mesh=mesh,
        in_specs=placed,
        out_specs=(P("gx", "gy", "gz"), P(None, ("gy", "gz"), "gx", None)),
        check_vma=False,
    )
```
